512 devices in a mesh: dp: 8 (over x, core), expert: 64 (over y, z).
Axes of the slice: x: 4, y: 8, z: 8, core: 2. Of those that a mesh axis runs over, the one named last changes fastest.
Arguments:
- cotangent: bfloat16 [65536, 3584], P(('dp', 'expert')), may hold values from -0.59765625 to 0.59765625
- expert_ids: int32 [65536, 1], P(('dp', 'expert')), may hold values from 0 to 15; in each aligned block of 128 rows (0 to 127, 128 to 255, ...) at most 12 rows name the same one
- route_weights: float32 [65536, 1], P(('dp', 'expert')), may hold values from 0.1 to 1
- gate_pre: bfloat16 [6144, 16384], P('dp', 'expert'), may hold values from -5 to 5
- up_pre: bfloat16 [6144, 16384], P('dp', 'expert'), may hold values from -5 to 5
- down_weight: bfloat16 [3584, 16384], P('dp', 'expert'), may hold values from -0.1875 to 0.1875
Outputs:
- weight_grad: bfloat16 [3584, 16384], P('dp', 'expert')
- gate_grad: bfloat16 [6144, 16384], P('dp', 'expert')
- up_grad: bfloat16 [6144, 16384], P('dp', 'expert')
The draws below stay inside these ranges and needn't reach their ends.
Inputs may be any that keep to these rules, and one draw needn't show every extreme that they name: `expert_ids`: each token names one expert. Among the tokens of one device, at most 12 name the same expert, and in every draw some expert is named by exactly 12 tokens of some device.
All inputs are finite; a program needn't handle non-finite values.
Results may differ from the reference program's by a relative error of at most 0.013.
Values may be sent and summed in bfloat16 or wider, within the bound.
No kernel may reach another device: no remote copies, remote signals or barrier semaphores. Data moves between devices by JAX's collectives and lax.ppermute only.
A program may use at most 64 MiB of HBM per device.

```python
import math
import jax
import jax.numpy as jnp
import numpy as np
from jax import lax

D = 3584
FFW = 1024
TOP = 1
TOK_DEV = 128
EXPERTS = 16
CAP = 12
TOKENS = 65536
SLOTS = 6144
N_DP = 8
N_EXPERT = 64


def shard_levels(own_key, extent, split, low, largest):
    def one(axis_at, parts):
        steps = jax.random.uniform(jax.random.fold_in(jax.random.fold_in(own_key, 6), axis_at), (parts,), jnp.float32, low / len(split), largest / len(split))
        return jnp.repeat(jnp.exp(steps), extent[axis_at] // parts).reshape((-1,) + (1,) * (len(extent) - axis_at - 1))

    gain = one(*split[0])
    for cut in split[1:]:
        gain = gain * one(*cut)
    return gain


def assign_block(own_key, own, number, rows, count, top, limit, skew):
    order = jax.random.permutation(own_key, count)
    heavy_load, common = load_shares(count, rows * top, limit, skew, True), load_shares(count, rows * top, limit, skew, False)
    places = jnp.arange(count)

    def named(lengths, turn):
        used = int((lengths > 0).sum())
        fixed = max(1, used // 4)
        shifted = fixed + (places - fixed + turn * (used - fixed)) % max(1, count - fixed)
        return jnp.zeros((count,), jnp.int32).at[order[jnp.where(places < fixed, places, shifted)]].set(jnp.asarray(lengths, jnp.int32))

    lengths = jnp.where(number % 4 == 0, named(heavy_load, number // 4), named(common, number - number // 4 - 1))
    mixed = jax.random.permutation(jax.random.fold_in(own, 3), count)
    source_of, receiver = mixed[0:count // 2 * 2:2], mixed[1:count // 2 * 2:2]
    room = jnp.minimum(lengths[source_of] - 1, limit - lengths[receiver]) // 2
    room = jnp.where((source_of == order[0]) | (receiver == order[0]) | (lengths[receiver] == 0), 0, jnp.maximum(room, 0))
    shifted = jax.random.randint(jax.random.fold_in(own, 4), (count // 2,), 0, 1 << 20) % (room + 1)
    lengths = lengths.at[source_of].add(-shifted).at[receiver].add(shifted)
    labels = jnp.searchsorted(jnp.cumsum(lengths), jnp.arange(rows * top), side="right").astype(jnp.int32)
    listing = labels.reshape(top, rows).T
    listing = listing[jax.random.permutation(jax.random.fold_in(own, 1), rows)]
    turn = jax.random.randint(jax.random.fold_in(own, 2), (rows, 1), 0, top)
    return jnp.take_along_axis(listing, (jnp.arange(top)[None, :] + turn) % top, axis=1)


def load_shares(count, total, most, lean, full):
    weights = [(1 << 20) // math.isqrt(standing ** lean) + 1 for standing in range(1, count + 1)]
    largest = most if full else min(most, max(-(-total // count), total * weights[0] // sum(weights)))
    least = 1 if total - largest >= count - 1 else 0
    holding, surplus = [largest] + [least] * (count - 1), total - largest - least * (count - 1)
    while surplus > 0:
        movable = [i for i in range(1, count) if holding[i] < largest] or [i for i in range(1, count) if holding[i] < most]
        whole, left = sum([weights[i] for i in movable]), surplus
        for i in movable:
            more = min(most - holding[i], max(1, left * weights[i] // whole), surplus)
            holding[i] = holding[i] + more
            surplus = surplus - more
    return np.array(holding)


def normal_values(rng, extent, width, limit, cuts=(), kind=jnp.bfloat16):
    drawn = width * jax.random.normal(rng, extent, jnp.float32)
    if cuts:
        drawn = drawn * shard_levels(rng, extent, cuts, -0.22, 0.18)
    return jnp.clip(drawn, -limit, limit).astype(kind)


def setup_inputs(seed: int = 0) -> dict:
    splits = jax.random.split(jax.random.key(seed), 7)
    cotangent = normal_values(splits[0], (TOKENS, D), 0.1, 0.59765625, ((0, 512),))
    expert_ids_keys = jax.random.split(jax.random.fold_in(splits[1], 1), TOKENS // TOK_DEV)
    expert_ids_turns = jax.random.permutation(jax.random.fold_in(splits[1], 3), TOKENS // TOK_DEV)
    expert_ids = jax.vmap(lambda own, number: assign_block(jax.random.fold_in(splits[1], 2), own, number, TOK_DEV, EXPERTS, TOP, CAP, 2))(expert_ids_keys, expert_ids_turns).reshape((TOKENS, TOP))
    route_weights = jnp.clip(0.1 + 0.9 * jax.random.uniform(splits[2], (TOKENS, TOP), jnp.float32) ** shard_levels(splits[2], (TOKENS, TOP), ((0, 512),), -0.2, 0.2), 0.1, 1.0)
    gate_pre = normal_values(splits[3], (SLOTS, EXPERTS * FFW), 1.0, 5.0, ((0, 8), (1, 64)))
    up_pre = normal_values(splits[4], (SLOTS, EXPERTS * FFW), 1.0, 5.0, ((0, 8), (1, 64)))
    down_weight = normal_values(splits[5], (D, EXPERTS * FFW), FFW ** -0.5, 0.1875, ((0, 8), (1, 64)))
    return {"cotangent": cotangent, "expert_ids": expert_ids, "route_weights": route_weights, "gate_pre": gate_pre, "up_pre": up_pre, "down_weight": down_weight}


def group_terms(cotangent, expert_ids, route_weights, gate_pre, up_pre, down_weight):
    onehot = (expert_ids[..., None] == jnp.arange(EXPERTS, dtype=jnp.int32)).astype(jnp.int32)
    touched = jnp.sum(onehot, axis=2)
    earlier = jnp.cumsum(touched, axis=1) - touched
    position = jnp.sum(onehot * earlier[:, :, None, :], axis=3)
    sources = jnp.arange(N_EXPERT, dtype=jnp.int32)[:, None, None] * CAP
    rows = (sources + position).astype(jnp.int32)
    scaled = route_weights[..., None] * cotangent.astype(jnp.float32)[:, :, None, :]
    routed = jnp.zeros((EXPERTS, N_EXPERT * CAP, D), jnp.float32).at[expert_ids, rows].add(scaled)
    routed_half = lax.optimization_barrier(routed.astype(jnp.bfloat16))
    routed_full = routed_half.astype(jnp.float32)
    weights = down_weight.astype(jnp.float32).reshape(D, EXPERTS, FFW)
    gate_full = gate_pre.astype(jnp.float32).reshape(N_EXPERT * CAP, EXPERTS, FFW)
    up_full = up_pre.astype(jnp.float32).reshape(N_EXPERT * CAP, EXPERTS, FFW)
    upstream = jnp.einsum('xrd,dxf->rxf', routed_full, weights)
    sigmoid = jax.nn.sigmoid(gate_full)
    active = gate_full * sigmoid
    product_half = lax.optimization_barrier((active * up_full).astype(jnp.bfloat16))
    gate_grad = (upstream * up_full * sigmoid * (1.0 + gate_full * (1.0 - sigmoid))).astype(jnp.bfloat16)
    up_grad = (upstream * active).astype(jnp.bfloat16)
    partial_sum = jnp.einsum('xrd,rxf->dxf', routed_full, product_half.astype(jnp.float32))
    partial_half = partial_sum.reshape(D, EXPERTS * FFW).astype(jnp.bfloat16)
    return partial_half, gate_grad.reshape(N_EXPERT * CAP, EXPERTS * FFW), up_grad.reshape(N_EXPERT * CAP, EXPERTS * FFW)


def reference(cotangent, expert_ids, route_weights, gate_pre, up_pre, down_weight):
    stacked = (cotangent.reshape(N_DP, N_EXPERT, TOK_DEV, D),
               expert_ids.reshape(N_DP, N_EXPERT, TOK_DEV, TOP),
               route_weights.reshape(N_DP, N_EXPERT, TOK_DEV, TOP),
               gate_pre.reshape(N_DP, N_EXPERT * CAP, EXPERTS * FFW),
               up_pre.reshape(N_DP, N_EXPERT * CAP, EXPERTS * FFW))

    def step(total, pieces):
        partial_half, gate_grad, up_grad = group_terms(pieces[0], pieces[1], pieces[2], pieces[3], pieces[4], down_weight)
        return total + partial_half.astype(jnp.float32), (gate_grad, up_grad)

    start = jnp.zeros((D, EXPERTS * FFW), jnp.float32)
    total, grads = lax.scan(step, start, stacked)
    weight_grad = total.astype(jnp.bfloat16)
    gate_grad = grads[0].reshape(SLOTS, EXPERTS * FFW)
    up_grad = grads[1].reshape(SLOTS, EXPERTS * FFW)
    return weight_grad, gate_grad, up_grad
```

```python
import jax
import jax.numpy as jnp
from jax import lax
from jax.experimental import pallas as pl
from jax.experimental.pallas import tpu as pltpu
from jax.sharding import PartitionSpec as P

CAP = 12
PART = 24
BF = jnp.bfloat16
F32 = jnp.float32
VMEM_LIMIT = 56 * 1024 * 1024


def expert_xor(value, mask):
    return lax.ppermute(value, "expert", [(i, i ^ mask) for i in range(lax.axis_size("expert"))])


def dp_xor(value, mask):
    return lax.ppermute(value, "dp", [(i, i ^ mask) for i in range(lax.axis_size("dp"))])


def swapped(value, flip):
    experts = lax.axis_size("expert")
    pairs = []
    for d in range(lax.axis_size("dp")):
        for s in range(experts):
            to_dp = (s & 1) * 4 + (d & 3)
            to_expert = (s & ~3) + (((s >> 1) & 1) ^ flip) * 2 + (d >> 2)
            pairs.append((d * experts + s, to_dp * experts + to_expert))
    return lax.ppermute(value, ("dp", "expert"), pairs)


def whole(shape):
    return pl.BlockSpec(memory_space=pltpu.VMEM)


SCALARS = pl.BlockSpec(memory_space=pltpu.SMEM)


def slots_body(ids_ref, weights_ref, cot_ref, out_ref):
    tokens = ids_ref.shape[1]
    experts = out_ref.shape[0]
    half = out_ref.shape[3]
    ids = jnp.broadcast_to(ids_ref[...].astype(F32), (tokens, tokens))
    row = lax.broadcasted_iota(jnp.int32, (tokens, tokens), 0)
    col = lax.broadcasted_iota(jnp.int32, (tokens, tokens), 1)
    ids_down = jnp.sum(jnp.where(row == col, ids, 0.0), axis=1, keepdims=True)
    earlier = jnp.where((ids_down == ids) & (row < col), 1.0, 0.0)
    position = jnp.sum(earlier, axis=0, keepdims=True)
    target = (ids_ref[...].astype(F32) * PART + position).astype(jnp.int32)
    place = lax.broadcasted_iota(jnp.int32, (experts * PART, tokens), 0)
    first = place == target
    second = place == target + CAP
    scale = jnp.sum(jnp.where(first | second, weights_ref[...], 0.0), axis=1, keepdims=True)
    picked = jnp.dot(
        first.astype(F32).astype(BF), cot_ref[:, :half], preferred_element_type=F32
    ) + jnp.dot(second.astype(F32).astype(BF), cot_ref[:, half:], preferred_element_type=F32)
    rows = picked * scale
    for x in range(experts):
        out_ref[x, 0] = rows[x * PART : (x + 1) * PART].astype(BF)


def slot_buffer(cotangent, expert_ids, route_weights, experts):
    tokens, width = cotangent.shape
    return pl.pallas_call(
        slots_body,
        grid=(2,),
        in_specs=[
            pl.BlockSpec((1, tokens), lambda k: (0, 0)),
            pl.BlockSpec((1, tokens), lambda k: (0, 0)),
            pl.BlockSpec((tokens, width // 2), lambda k: (0, k)),
        ],
        out_specs=pl.BlockSpec((experts, 1, PART, width // 4), lambda k: (0, k, 0, 0)),
        out_shape=jax.ShapeDtypeStruct((experts, 2, PART, width // 4), BF),
        compiler_params=pltpu.CompilerParams(vmem_limit_bytes=VMEM_LIMIT),
        name="slots",
    )(expert_ids.reshape(1, tokens), route_weights.reshape(1, tokens), cotangent)


def weight_body(s_ref, recv_ref, p0, p1, p2, p3, rows_ref, grad_ref):
    a1, a0, core, k = s_ref[0], s_ref[1], s_ref[2], s_ref[3]
    sources = recv_ref.shape[0]
    for b in range(2):
        for s in range(sources):
            rows_ref[b, s * CAP : (s + 1) * CAP, :] = recv_ref[s, b * CAP : (b + 1) * CAP, :]
    block = grad_ref.shape[4]
    for b in range(2):
        for q, piece in enumerate((p0, p1, p2, p3)):
            e, d = q >> 1, q & 1
            grad = lax.dot_general(
                rows_ref[b], piece[...], (((0,), (0,)), ((), ())), preferred_element_type=F32
            ).astype(BF)
            for c in range(2):
                grad_ref[c ^ core, d ^ k ^ a1, b ^ a0, e] = grad[c * block : (c + 1) * block]


def weight_partial(scalars, recv, pieces, block):
    sources, _, half = recv.shape
    count = sources * CAP
    columns = pieces[0].shape[1]
    return pl.pallas_call(
        weight_body,
        in_specs=[SCALARS, whole(recv.shape)] + [whole((count, columns))] * 4,
        out_specs=[whole((2, count, half)), whole((2, 2, 2, 2, block, columns))],
        out_shape=[
            jax.ShapeDtypeStruct((2, count, half), BF),
            jax.ShapeDtypeStruct((2, 2, 2, 2, block, columns), BF),
        ],
        compiler_params=pltpu.CompilerParams(vmem_limit_bytes=VMEM_LIMIT),
        name="weight_partial",
    )(scalars, recv, *pieces)


def upstream_body(s_ref, rows_ref, near_ref, far_ref, c0, c1, c2, c3):
    a1, a0, core, k = s_ref[0], s_ref[1], s_ref[2], s_ref[3]
    for q, out in enumerate((c0, c1, c2, c3)):
        e, d = q >> 1, q & 1
        total = None
        for b in range(2):
            near = near_ref[d ^ k ^ a1, b ^ a0, e]
            far = far_ref[d ^ k ^ a1, b ^ a0, e]
            low = jnp.where(core == 0, near, far)
            high = jnp.where(core == 0, far, near)
            part = jnp.dot(
                rows_ref[b], jnp.concatenate([low, high], axis=0), preferred_element_type=F32
            )
            total = part if total is None else total + part
        out[...] = total.astype(out.dtype)


def upstream_partial(scalars, rows, near, far):
    count = rows.shape[1]
    columns = near.shape[-1]
    return pl.pallas_call(
        upstream_body,
        in_specs=[SCALARS, whole(rows.shape), whole(near.shape), whole(far.shape)],
        out_specs=[whole((count, columns))] * 4,
        out_shape=[jax.ShapeDtypeStruct((count, columns), F32)]
        + [jax.ShapeDtypeStruct((count, columns), BF)] * 3,
        compiler_params=pltpu.CompilerParams(vmem_limit_bytes=VMEM_LIMIT),
        name="upstream_partial",
    )(scalars, rows, near, far)


def finish_body(s_ref, gate_ref, up_ref, c0, r1, r2, r3, gate_out, up_out):
    group = s_ref[4]
    for side in range(2):
        for t in range(2):
            if side == 0:
                part = c0[:, t] + r1[:, t].astype(F32)
            else:
                part = r2[:, t].astype(F32) + r3[:, t].astype(F32)
            inner = (group ^ side) == 0
            index = jnp.where(inner, 3 * t, 1 + t)
            gate = gate_ref[:, index].astype(F32)
            up = up_ref[:, index].astype(F32)
            sigmoid = jax.nn.sigmoid(gate)
            gate_out[:, index] = (part * up * sigmoid * (1.0 + gate * (1.0 - sigmoid))).astype(BF)
            up_out[:, index] = (part * (gate * sigmoid)).astype(BF)


def finish(scalars, gate, up, c0, r1, r2, r3):
    full = whole(gate.shape)
    part = whole(c0.shape)
    return pl.pallas_call(
        finish_body,
        in_specs=[SCALARS, full, full, part, part, part, part],
        out_specs=[full, full],
        out_shape=[jax.ShapeDtypeStruct(gate.shape, BF)] * 2,
        compiler_params=pltpu.CompilerParams(vmem_limit_bytes=VMEM_LIMIT),
        name="finish",
    )(scalars, gate, up, c0, r1, r2, r3)


def per_device(cotangent, expert_ids, route_weights, gate_pre, up_pre, down_weight):
    devices = lax.axis_size("expert")
    experts = devices // 4
    ys = devices // 8
    columns = gate_pre.shape[1]
    block = down_weight.shape[0]
    dp = lax.axis_index("dp")
    place = lax.axis_index("expert")
    a1, a0, core = dp >> 2, (dp >> 1) & 1, dp & 1
    half, line, k = (place >> 2) & 1, (place >> 1) & 1, place & 1
    group = half ^ line
    scalars = jnp.stack([a1, a0, core, k, group]).astype(jnp.int32)

    own = jnp.stack([swapped(down_weight, 0), swapped(down_weight, 1)])
    own, cotangent = lax.optimization_barrier((own, cotangent))

    slots = slot_buffer(cotangent, expert_ids, route_weights, experts)
    lists = [
        [y * 8 + z for y in range(ys) for z in zs] for zs in ((0, 1, 6, 7), (2, 3, 4, 5))
    ]
    recv = lax.all_to_all(
        slots.reshape(devices // 2, PART, slots.shape[3]),
        "expert",
        split_axis=0,
        concat_axis=0,
        tiled=True,
        axis_index_groups=lists,
    )

    gate4 = gate_pre.reshape(ys, 4, PART, columns)
    up4 = up_pre.reshape(ys, 4, PART, columns)
    gate_full = gate4.astype(F32)
    product = (gate_full * jax.nn.sigmoid(gate_full) * up4.astype(F32)).astype(BF)
    outer = jnp.concatenate([product[:, 0:1], product[:, 3:4]], axis=1)
    inner = product[:, 1:3]
    mine = jnp.where(group == 0, outer, inner).reshape(-1, columns)
    theirs = jnp.where(group == 0, inner, outer).reshape(-1, columns)
    pieces = [mine, expert_xor(mine, 1), expert_xor(theirs, 2), expert_xor(theirs, 3)]

    near = jnp.stack([own, dp_xor(own, 2), dp_xor(own, 4), dp_xor(own, 6)])
    far = dp_xor(near, 1)
    near = near.reshape(2, 2, 2, block, columns)
    far = far.reshape(2, 2, 2, block, columns)

    recv, near, far = lax.optimization_barrier((recv, near, far))
    rows, grad = weight_partial(scalars, recv, pieces, block)
    crossed = dp_xor(grad[1], 1)
    c0, c1, c2, c3 = upstream_partial(scalars, rows, near, far)
    summed = (grad[0].astype(F32) + crossed.astype(F32)).astype(BF)
    kept = summed[0, 0].astype(F32)
    for mask, piece in ((2, summed[0, 1]), (4, summed[1, 0]), (6, summed[1, 1])):
        kept = kept + dp_xor(piece, mask).astype(F32)
    kept = kept.astype(BF)
    weight_grad = (
        swapped(kept[0], 0).astype(F32) + swapped(kept[1], 1).astype(F32)
    ).astype(BF)

    shape = (ys, 2, PART, columns)
    r1, r2, r3 = (expert_xor(c, q) for q, c in ((1, c1), (2, c2), (3, c3)))
    gate_grad, up_grad = finish(
        scalars,
        gate4,
        up4,
        c0.reshape(shape),
        r1.reshape(shape),
        r2.reshape(shape),
        r3.reshape(shape),
    )
    return (weight_grad, gate_grad.reshape(gate_pre.shape), up_grad.reshape(up_pre.shape))


def solution(mesh):
    placed = (
        P(("dp", "expert"), None),
        P(("dp", "expert"), None),
        P(("dp", "expert"), None),
        P("dp", "expert"),
        P("dp", "expert"),
        P("dp", "expert"),
    )
    return jax.shard_map(
        per_device,
        mesh=mesh,
        in_specs=placed,
        out_specs=(P("dp", "expert"), P("dp", "expert"), P("dp", "expert")),
        check_vma=False,
    )
```

```python
import jax
import jax.numpy as jnp
from jax import lax
from jax.experimental import pallas as pl
from jax.experimental.pallas import tpu as pltpu
from jax.sharding import PartitionSpec as P


CAP = 12
PART = 24
BF = jnp.bfloat16
F32 = jnp.float32
VMEM_LIMIT = 16 * 1024 * 1024


def expert_xor(value, mask):
    return lax.ppermute(value, "expert", [(i, i ^ mask) for i in range(lax.axis_size("expert"))])


def dp_xor(value, mask):
    return lax.ppermute(value, "dp", [(i, i ^ mask) for i in range(lax.axis_size("dp"))])


def swapped(value, flip):
    experts = lax.axis_size("expert")
    pairs = []
    for d in range(lax.axis_size("dp")):
        for s in range(experts):
            to_dp = (s & 1) * 4 + (d & 3)
            to_expert = (s & ~3) + (((s >> 1) & 1) ^ flip) * 2 + (d >> 2)
            pairs.append((d * experts + s, to_dp * experts + to_expert))
    return lax.ppermute(value, ("dp", "expert"), pairs)


SCALARS = pl.BlockSpec(memory_space=pltpu.SMEM)
WHOLE = pl.BlockSpec(memory_space=pltpu.VMEM)
PARAMS = pltpu.CompilerParams(vmem_limit_bytes=VMEM_LIMIT)


def cost(flops, size):
    return pl.CostEstimate(flops=flops, transcendentals=0, bytes_accessed=size)


def slots_body(ids_ref, weights_ref, cot_ref, out_ref):
    tokens = ids_ref.shape[1]
    experts = out_ref.shape[0]
    half = out_ref.shape[3]
    ids = jnp.broadcast_to(ids_ref[...].astype(F32), (tokens, tokens))
    row = lax.broadcasted_iota(jnp.int32, (tokens, tokens), 0)
    col = lax.broadcasted_iota(jnp.int32, (tokens, tokens), 1)
    ids_down = jnp.sum(jnp.where(row == col, ids, 0.0), axis=1, keepdims=True)
    earlier = jnp.where((ids_down == ids) & (row < col), 1.0, 0.0)
    position = jnp.sum(earlier, axis=0, keepdims=True)
    target = (ids_ref[...].astype(F32) * PART + position).astype(jnp.int32)
    place = lax.broadcasted_iota(jnp.int32, (experts * PART, tokens), 0)
    first = place == target
    second = place == target + CAP
    scale = jnp.sum(jnp.where(first | second, weights_ref[...], 0.0), axis=1, keepdims=True)
    picked = jnp.dot(
        first.astype(F32).astype(BF), cot_ref[:, :half], preferred_element_type=F32
    ) + jnp.dot(second.astype(F32).astype(BF), cot_ref[:, half:], preferred_element_type=F32)
    rows = picked * scale
    for x in range(experts):
        out_ref[x, 0] = rows[x * PART : (x + 1) * PART].astype(BF)


def slot_buffer(cotangent, expert_ids, route_weights, experts):
    tokens, width = cotangent.shape
    return pl.pallas_call(
        slots_body,
        grid=(2,),
        in_specs=[
            pl.BlockSpec((1, tokens), lambda k: (0, 0)),
            pl.BlockSpec((1, tokens), lambda k: (0, 0)),
            pl.BlockSpec((tokens, width // 2), lambda k: (0, k)),
        ],
        out_specs=pl.BlockSpec((experts, 1, PART, width // 4), lambda k: (0, k, 0, 0)),
        out_shape=jax.ShapeDtypeStruct((experts, 2, PART, width // 4), BF),
        compiler_params=PARAMS,
        cost_estimate=cost(4 * tokens * experts * PART * width, 4 * tokens * width),
        name="slots",
    )(
        *(
            pltpu.with_memory_space_constraint(value, pltpu.HBM)
            for value in (
                expert_ids.reshape(1, tokens),
                route_weights.reshape(1, tokens),
                cotangent,
            )
        )
    )


def product_body(s_ref, gate_ref, up_ref, out_ref):
    group = s_ref[4]
    for t in range(4):
        gate = gate_ref[:, t].astype(F32)
        value = (gate * jax.nn.sigmoid(gate) * up_ref[:, t].astype(F32)).astype(BF)
        side = group ^ (0 if t in (0, 3) else 1)
        out_ref[side, :, t >> 1] = value


def products(scalars, gate, up):
    ys, _, part, columns = gate.shape
    return pl.pallas_call(
        product_body,
        in_specs=[SCALARS, WHOLE, WHOLE],
        out_specs=WHOLE,
        out_shape=jax.ShapeDtypeStruct((2, ys, 2, part, columns), BF),
        compiler_params=PARAMS,
        cost_estimate=cost(gate.size * 200, gate.size * 8),
        name="products",
    )(scalars, gate, up)


def slot_of(e, r1, r0):
    near, far = ((4, 0), (1, 5)) if e == 0 else ((6, 7), (3, 2))
    return jnp.where(r1 == 0, jnp.where(r0 == 0, *near), jnp.where(r0 == 0, *far))


def weight_body(s_ref, recv_ref, p0, p1, p2, p3, rows_ref, keep_ref, send_ref):
    core, k, a1, a0 = s_ref[0], s_ref[1], s_ref[2], s_ref[3]
    sources = recv_ref.shape[0]
    block = keep_ref.shape[1]
    for b in range(2):
        for s in range(sources):
            rows_ref[b, s * CAP : (s + 1) * CAP, :] = recv_ref[s, b * CAP : (b + 1) * CAP, :]
    for b in range(2):
        for q, piece in enumerate((p0, p1, p2, p3)):
            grad = lax.dot_general(
                rows_ref[b], piece[...], (((0,), (0,)), ((), ())), preferred_element_type=F32
            ).astype(BF)
            low, high = grad[:block], grad[block:]
            place = slot_of(q >> 1, (q & 1) ^ k ^ a1, b ^ a0)
            keep_ref[place] = jnp.where(core == 0, low, high)
            send_ref[place] = jnp.where(core == 0, high, low)


def weight_partial(scalars, recv, pieces, block):
    sources, _, half = recv.shape
    count = sources * CAP
    columns = pieces[0].shape[1]
    grad = jax.ShapeDtypeStruct((8, block, columns), BF)
    return pl.pallas_call(
        weight_body,
        in_specs=[SCALARS] + [WHOLE] * 5,
        out_specs=[WHOLE] * 3,
        out_shape=[jax.ShapeDtypeStruct((2, count, half), BF), grad, grad],
        compiler_params=PARAMS,
        cost_estimate=cost(16 * count * half * columns, 8 * count * half),
        name="weight_partial",
    )(scalars, recv, *pieces)


def upstream_body(s_ref, rows_ref, near_ref, far_ref, *out_refs):
    core, k, a1, a0 = s_ref[0], s_ref[1], s_ref[2], s_ref[3]
    for q in range(4):
        total = None
        for b in range(2):
            near = near_ref[((q & 1) ^ k ^ a1) * 2 + (b ^ a0), q >> 1]
            far = far_ref[((q & 1) ^ k ^ a1) * 2 + (b ^ a0), q >> 1]
            low = jnp.where(core == 0, near, far)
            high = jnp.where(core == 0, far, near)
            part = jnp.dot(
                rows_ref[b], jnp.concatenate([low, high], axis=0), preferred_element_type=F32
            )
            total = part if total is None else total + part
        out_refs[q][...] = total.astype(BF)


def upstream_partial(scalars, rows, near, far):
    _, count, half = rows.shape
    columns = near.shape[-1]
    return pl.pallas_call(
        upstream_body,
        in_specs=[SCALARS, WHOLE, WHOLE, WHOLE],
        out_specs=[WHOLE] * 4,
        out_shape=[jax.ShapeDtypeStruct((count, columns), BF)] * 4,
        compiler_params=PARAMS,
        cost_estimate=cost(16 * count * half * columns, 8 * count * half),
        name="upstream_partial",
    )(scalars, rows, near, far)


def finish_body(s_ref, gate_ref, up_ref, c0, c1, c2, c3, gate_out, up_out):
    group = s_ref[4]
    for side in range(2):
        for t in range(2):
            left, right = ((c0, c1), (c2, c3))[side]
            part = left[:, t].astype(F32) + right[:, t].astype(F32)
            index = jnp.where((group ^ side) == 0, 3 * t, 1 + t)
            gate = gate_ref[:, index].astype(F32)
            up = up_ref[:, index].astype(F32)
            sigmoid = jax.nn.sigmoid(gate)
            gate_out[:, index] = (part * up * sigmoid * (1.0 + gate * (1.0 - sigmoid))).astype(BF)
            up_out[:, index] = (part * (gate * sigmoid)).astype(BF)


def finish(scalars, gate, up, parts):
    return pl.pallas_call(
        finish_body,
        in_specs=[SCALARS] + [WHOLE] * 6,
        out_specs=[WHOLE] * 2,
        out_shape=[jax.ShapeDtypeStruct(gate.shape, BF)] * 2,
        compiler_params=PARAMS,
        cost_estimate=cost(gate.size * 200, gate.size * 12),
        name="finish",
    )(scalars, gate, up, *parts)


def added(left, right):
    return (left.astype(F32) + right.astype(F32)).astype(BF)


def dispatched(slots):
    ys = lax.axis_size("expert") // 8
    lists = [[y * 8 + z for y in range(ys) for z in zs] for zs in ((0, 1, 6, 7), (2, 3, 4, 5))]
    return lax.all_to_all(
        slots, "expert", split_axis=0, concat_axis=0, tiled=True, axis_index_groups=lists
    )


def per_device(cotangent, expert_ids, route_weights, gate_pre, up_pre, down_weight):
    devices = lax.axis_size("expert")
    experts = devices // 4
    ys = devices // 8
    columns = gate_pre.shape[1]
    block = down_weight.shape[0]
    dp = lax.axis_index("dp")
    place = lax.axis_index("expert")
    group = ((place >> 2) ^ (place >> 1)) & 1
    scalars = jnp.stack([dp & 1, place & 1, dp >> 2, (dp >> 1) & 1, group]).astype(jnp.int32)
    gate4 = gate_pre.reshape(ys, 4, PART, columns)
    up4 = up_pre.reshape(ys, 4, PART, columns)

    own = [swapped(down_weight, flip) for flip in range(2)]
    sent = products(scalars, gate4, up4).reshape(2, -1, columns)
    slots = slot_buffer(cotangent, expert_ids, route_weights, experts)
    recv = dispatched(slots.reshape(devices // 2, PART, slots.shape[3]))
    pieces = [sent[0]] + [expert_xor(sent[q >> 1], q) for q in (1, 2, 3)]
    own = jnp.stack(own)
    near = jnp.stack([own] + [dp_xor(own, mask) for mask in (2, 4, 6)])
    far = dp_xor(near, 1)

    recv, near, far = lax.optimization_barrier((recv, near, far))
    rows, keep, send = weight_partial(scalars, recv, pieces, block)
    crossed = dp_xor(send, 1)
    parts = upstream_partial(scalars, rows, near, far)
    summed = added(keep, crossed)
    first = [dp_xor(summed[0:2], 2), dp_xor(summed[2:4], 6)]
    parts = [parts[0]] + [expert_xor(parts[q], q) for q in (1, 2, 3)]
    parts = [part.reshape(ys, 2, PART, columns) for part in parts]
    first = [added(summed[4:6], first[0]), added(summed[6:8], first[1])]
    second = [dp_xor(first[0][1], 6), dp_xor(first[1][1], 2)]
    kept = [added(first[e][0], second[e]) for e in range(2)]
    weight_grad = added(swapped(kept[0], 0), swapped(kept[1], 1))
    gate_grad, up_grad = finish(scalars, gate4, up4, parts)
    return (
        weight_grad,
        gate_grad.reshape(gate_pre.shape),
        up_grad.reshape(up_pre.shape),
    )


def solution(mesh):
    placed = (
        P(("dp", "expert"), None),
        P(("dp", "expert"), None),
        P(("dp", "expert"), None),
        P("dp", "expert"),
        P("dp", "expert"),
        P("dp", "expert"),
    )
    return jax.shard_map(
        per_device,
        mesh=mesh,
        in_specs=placed,
        out_specs=(P("dp", "expert"), P("dp", "expert"), P("dp", "expert")),
        check_vma=False,
    )
```

```python
import jax
import jax.numpy as jnp
from jax import lax
from jax.experimental import pallas as pl
from jax.experimental.pallas import tpu as pltpu
from jax.sharding import PartitionSpec as P


CAP = 12
PART = 24
BF = jnp.bfloat16
F32 = jnp.float32
VMEM_LIMIT = 16 * 1024 * 1024


def expert_xor(value, mask):
    return lax.ppermute(value, "expert", [(i, i ^ mask) for i in range(lax.axis_size("expert"))])


def dp_xor(value, mask):
    return lax.ppermute(value, "dp", [(i, i ^ mask) for i in range(lax.axis_size("dp"))])


def swapped(value, flip, back):
    experts = lax.axis_size("expert")
    pairs = []
    for d in range(lax.axis_size("dp")):
        for s in range(experts):
            high = d >> 2
            to_dp = ((s & 1) ^ high) * 4 + (d & 3)
            to_expert = (s & ~3) + (((s >> 1) & 1) ^ flip) * 2 + high
            pairs.append((d * experts + s, to_dp * experts + to_expert))
    if back:
        pairs = [(target, source) for source, target in pairs]
    return lax.ppermute(value, ("dp", "expert"), pairs)


SCALARS = pl.BlockSpec(memory_space=pltpu.SMEM)
WHOLE = pl.BlockSpec(memory_space=pltpu.VMEM)
PARAMS = pltpu.CompilerParams(vmem_limit_bytes=VMEM_LIMIT)


def cost(flops, size):
    return pl.CostEstimate(flops=flops, transcendentals=0, bytes_accessed=size)


def slots_body(ids_ref, weights_ref, cot_ref, out_ref):
    tokens = ids_ref.shape[1]
    experts = out_ref.shape[0]
    half = out_ref.shape[3]
    ids = jnp.broadcast_to(ids_ref[...].astype(F32), (tokens, tokens))
    row = lax.broadcasted_iota(jnp.int32, (tokens, tokens), 0)
    col = lax.broadcasted_iota(jnp.int32, (tokens, tokens), 1)
    ids_down = jnp.sum(jnp.where(row == col, ids, 0.0), axis=1, keepdims=True)
    earlier = jnp.where((ids_down == ids) & (row < col), 1.0, 0.0)
    position = jnp.sum(earlier, axis=0, keepdims=True)
    target = (ids_ref[...].astype(F32) * PART + position).astype(jnp.int32)
    place = lax.broadcasted_iota(jnp.int32, (experts * PART, tokens), 0)
    first = place == target
    second = place == target + CAP
    scale = jnp.sum(jnp.where(first | second, weights_ref[...], 0.0), axis=1, keepdims=True)
    picked = jnp.dot(
        first.astype(F32).astype(BF), cot_ref[:, :half], preferred_element_type=F32
    ) + jnp.dot(second.astype(F32).astype(BF), cot_ref[:, half:], preferred_element_type=F32)
    rows = picked * scale
    for x in range(experts):
        out_ref[x, 0] = rows[x * PART : (x + 1) * PART].astype(BF)


def slot_buffer(cotangent, expert_ids, route_weights, experts):
    tokens, width = cotangent.shape
    return pl.pallas_call(
        slots_body,
        grid=(2,),
        in_specs=[
            pl.BlockSpec((1, tokens), lambda k: (0, 0)),
            pl.BlockSpec((1, tokens), lambda k: (0, 0)),
            pl.BlockSpec((tokens, width // 2), lambda k: (0, k)),
        ],
        out_specs=pl.BlockSpec((experts, 1, PART, width // 4), lambda k: (0, k, 0, 0)),
        out_shape=jax.ShapeDtypeStruct((experts, 2, PART, width // 4), BF),
        compiler_params=PARAMS,
        cost_estimate=cost(4 * tokens * experts * PART * width, 4 * tokens * width),
        name="slots",
    )(
        *(
            pltpu.with_memory_space_constraint(value, pltpu.HBM)
            for value in (
                expert_ids.reshape(1, tokens),
                route_weights.reshape(1, tokens),
                cotangent,
            )
        )
    )


def product_body(s_ref, gate_ref, up_ref, out_ref):
    group = s_ref[3]
    for t in range(4):
        gate = gate_ref[:, t].astype(F32)
        value = (gate * jax.nn.sigmoid(gate) * up_ref[:, t].astype(F32)).astype(BF)
        side = group ^ (0 if t in (0, 3) else 1)
        out_ref[side, :, t >> 1] = value


def products(scalars, gate, up):
    ys, _, part, columns = gate.shape
    return pl.pallas_call(
        product_body,
        in_specs=[SCALARS, WHOLE, WHOLE],
        out_specs=WHOLE,
        out_shape=jax.ShapeDtypeStruct((2, ys, 2, part, columns), BF),
        compiler_params=PARAMS,
        cost_estimate=cost(gate.size * 200, gate.size * 8),
        name="products",
    )(scalars, gate, up)


def picked(near, far, r1, r0):
    return jnp.where(r1 == 0, jnp.where(r0 == 0, *near), jnp.where(r0 == 0, *far))


def slot_of(e, r1, r0):
    return picked(*(((4, 0), (1, 5)) if e == 0 else ((6, 7), (3, 2))), r1, r0)


def gathered_slot(e, r1, r0):
    return picked(*(((0, 2), (5, 4)) if e == 0 else ((1, 6), (7, 3))), r1, r0)


def weight_body(s_ref, recv_ref, p0, p1, p2, p3, rows_ref, keep_ref, send_ref):
    core, a1, a0 = s_ref[0], s_ref[1], s_ref[2]
    sources = recv_ref.shape[0]
    block = keep_ref.shape[1]
    for b in range(2):
        for s in range(sources):
            rows_ref[b, s * CAP : (s + 1) * CAP, :] = recv_ref[s, b * CAP : (b + 1) * CAP, :]
    for b in range(2):
        for q, piece in enumerate((p0, p1, p2, p3)):
            grad = lax.dot_general(
                rows_ref[b], piece[...], (((0,), (0,)), ((), ())), preferred_element_type=F32
            ).astype(BF)
            low, high = grad[:block], grad[block:]
            place = slot_of(q >> 1, (q & 1) ^ a1, b ^ a0)
            keep_ref[place] = jnp.where(core == 0, low, high)
            send_ref[place] = jnp.where(core == 0, high, low)


def weight_partial(scalars, recv, pieces, block):
    sources, _, half = recv.shape
    count = sources * CAP
    columns = pieces[0].shape[1]
    grad = jax.ShapeDtypeStruct((8, block, columns), BF)
    return pl.pallas_call(
        weight_body,
        in_specs=[SCALARS] + [WHOLE] * 5,
        out_specs=[WHOLE] * 3,
        out_shape=[jax.ShapeDtypeStruct((2, count, half), BF), grad, grad],
        compiler_params=PARAMS,
        cost_estimate=cost(16 * count * half * columns, 8 * count * half),
        name="weight_partial",
    )(scalars, recv, *pieces)


def upstream_body(s_ref, rows_ref, near_ref, far_ref, *out_refs):
    core, a1, a0 = s_ref[0], s_ref[1], s_ref[2]
    for q in range(4):
        total = None
        for b in range(2):
            near = near_ref[gathered_slot(q >> 1, (q & 1) ^ a1, b ^ a0)]
            far = far_ref[gathered_slot(q >> 1, (q & 1) ^ a1, b ^ a0)]
            low = jnp.where(core == 0, near, far)
            high = jnp.where(core == 0, far, near)
            part = jnp.dot(
                rows_ref[b], jnp.concatenate([low, high], axis=0), preferred_element_type=F32
            )
            total = part if total is None else total + part
        out_refs[q][...] = total.astype(BF)


def upstream_partial(scalars, rows, near, far):
    _, count, half = rows.shape
    columns = near.shape[-1]
    return pl.pallas_call(
        upstream_body,
        in_specs=[SCALARS, WHOLE, WHOLE, WHOLE],
        out_specs=[WHOLE] * 4,
        out_shape=[jax.ShapeDtypeStruct((count, columns), BF)] * 4,
        compiler_params=PARAMS,
        cost_estimate=cost(16 * count * half * columns, 8 * count * half),
        name="upstream_partial",
    )(scalars, rows, near, far)


def finish_body(s_ref, gate_ref, up_ref, c0, c1, c2, c3, gate_out, up_out):
    group = s_ref[3]
    for side in range(2):
        for t in range(2):
            left, right = ((c0, c1), (c2, c3))[side]
            part = left[:, t].astype(F32) + right[:, t].astype(F32)
            index = jnp.where((group ^ side) == 0, 3 * t, 1 + t)
            gate = gate_ref[:, index].astype(F32)
            up = up_ref[:, index].astype(F32)
            sigmoid = jax.nn.sigmoid(gate)
            gate_out[:, index] = (part * up * sigmoid * (1.0 + gate * (1.0 - sigmoid))).astype(BF)
            up_out[:, index] = (part * (gate * sigmoid)).astype(BF)


def finish(scalars, gate, up, parts):
    return pl.pallas_call(
        finish_body,
        in_specs=[SCALARS] + [WHOLE] * 6,
        out_specs=[WHOLE] * 2,
        out_shape=[jax.ShapeDtypeStruct(gate.shape, BF)] * 2,
        compiler_params=PARAMS,
        cost_estimate=cost(gate.size * 200, gate.size * 12),
        name="finish",
    )(scalars, gate, up, *parts)


def added(left, right):
    return (left.astype(F32) + right.astype(F32)).astype(BF)


def dispatched(slots):
    ys = lax.axis_size("expert") // 8
    lists = [[y * 8 + z for y in range(ys) for z in zs] for zs in ((0, 1, 6, 7), (2, 3, 4, 5))]
    return lax.all_to_all(
        slots, "expert", split_axis=0, concat_axis=0, tiled=True, axis_index_groups=lists
    )


def per_device(cotangent, expert_ids, route_weights, gate_pre, up_pre, down_weight):
    devices = lax.axis_size("expert")
    experts = devices // 4
    ys = devices // 8
    columns = gate_pre.shape[1]
    block = down_weight.shape[0]
    dp = lax.axis_index("dp")
    place = lax.axis_index("expert")
    group = ((place >> 2) ^ (place >> 1)) & 1
    scalars = jnp.stack([dp & 1, dp >> 2, (dp >> 1) & 1, group]).astype(jnp.int32)
    gate4 = gate_pre.reshape(ys, 4, PART, columns)
    up4 = up_pre.reshape(ys, 4, PART, columns)

    own = [swapped(down_weight, flip, False) for flip in range(2)]
    sent = products(scalars, gate4, up4).reshape(2, -1, columns)
    pieces = [sent[0]] + [expert_xor(sent[q >> 1], q) for q in (1, 2, 3)]
    slots = slot_buffer(cotangent, expert_ids, route_weights, experts)
    recv = dispatched(slots.reshape(devices // 2, PART, slots.shape[3]))
    own = [value[None] for value in own]
    ahead, behind = dp_xor(own[0], 2), dp_xor(own[1], 6)
    low = dp_xor(jnp.concatenate([own[0], ahead]), 6)
    high = dp_xor(jnp.concatenate([own[1], behind]), 2)
    near = jnp.concatenate(own + [ahead, behind, low, high])
    far = dp_xor(near, 1)

    recv, near = lax.optimization_barrier((recv, near))
    rows, keep, send = weight_partial(scalars, recv, pieces, block)
    crossed = dp_xor(send, 1)
    parts = upstream_partial(scalars, rows, near, far)
    summed = added(keep, crossed)
    first = [dp_xor(summed[0:2], 2), dp_xor(summed[2:4], 6)]
    parts = [parts[0]] + [expert_xor(parts[q], q) for q in (1, 2, 3)]
    parts = [part.reshape(ys, 2, PART, columns) for part in parts]
    first = [added(summed[4:6], first[0]), added(summed[6:8], first[1])]
    second = [dp_xor(first[0][1], 6), dp_xor(first[1][1], 2)]
    kept = [added(first[e][0], second[e]) for e in range(2)]
    weight_grad = added(swapped(kept[0], 0, True), swapped(kept[1], 1, True))
    gate_grad, up_grad = finish(scalars, gate4, up4, parts)
    return (
        weight_grad,
        gate_grad.reshape(gate_pre.shape),
        up_grad.reshape(up_pre.shape),
    )


def solution(mesh):
    placed = (
        P(("dp", "expert"), None),
        P(("dp", "expert"), None),
        P(("dp", "expert"), None),
        P("dp", "expert"),
        P("dp", "expert"),
        P("dp", "expert"),
    )
    return jax.shard_map(
        per_device,
        mesh=mesh,
        in_specs=placed,
        out_specs=(P("dp", "expert"), P("dp", "expert"), P("dp", "expert")),
        check_vma=False,
    )
```

```python
import jax
import jax.numpy as jnp
from jax import lax
from jax.experimental import pallas as pl
from jax.experimental.pallas import tpu as pltpu
from jax.sharding import PartitionSpec as P


CAP = 12
PART = 24
BF = jnp.bfloat16
F32 = jnp.float32
VMEM_LIMIT = 16 * 1024 * 1024


def expert_xor(value, mask):
    return lax.ppermute(value, "expert", [(i, i ^ mask) for i in range(lax.axis_size("expert"))])


def dp_xor(value, mask):
    return lax.ppermute(value, "dp", [(i, i ^ mask) for i in range(lax.axis_size("dp"))])


def swapped(value, flip, back):
    experts = lax.axis_size("expert")
    pairs = []
    for d in range(lax.axis_size("dp")):
        for s in range(experts):
            high = d >> 2
            to_dp = ((s & 1) ^ high ^ (d & 1)) * 4 + (d & 3)
            to_expert = (s & ~3) + (((s >> 1) & 1) ^ flip) * 2 + high
            pairs.append((d * experts + s, to_dp * experts + to_expert))
    if back:
        pairs = [(target, source) for source, target in pairs]
    return lax.ppermute(value, ("dp", "expert"), pairs)


SCALARS = pl.BlockSpec(memory_space=pltpu.SMEM)
WHOLE = pl.BlockSpec(memory_space=pltpu.VMEM)
PARAMS = pltpu.CompilerParams(vmem_limit_bytes=VMEM_LIMIT)


def cost(flops, size):
    return pl.CostEstimate(flops=flops, transcendentals=0, bytes_accessed=size)


def slots_body(ids_ref, weights_ref, cot_ref, out_ref):
    tokens = ids_ref.shape[1]
    experts = out_ref.shape[0]
    half = out_ref.shape[3]
    ids = jnp.broadcast_to(ids_ref[...].astype(F32), (tokens, tokens))
    row = lax.broadcasted_iota(jnp.int32, (tokens, tokens), 0)
    col = lax.broadcasted_iota(jnp.int32, (tokens, tokens), 1)
    ids_down = jnp.sum(jnp.where(row == col, ids, 0.0), axis=1, keepdims=True)
    earlier = jnp.where((ids_down == ids) & (row < col), 1.0, 0.0)
    position = jnp.sum(earlier, axis=0, keepdims=True)
    target = (ids_ref[...].astype(F32) * PART + position).astype(jnp.int32)
    place = lax.broadcasted_iota(jnp.int32, (experts * PART, tokens), 0)
    first = place == target
    second = place == target + CAP
    scale = jnp.sum(jnp.where(first | second, weights_ref[...], 0.0), axis=1, keepdims=True)
    picked = jnp.dot(
        first.astype(F32).astype(BF), cot_ref[:, :half], preferred_element_type=F32
    ) + jnp.dot(second.astype(F32).astype(BF), cot_ref[:, half:], preferred_element_type=F32)
    rows = picked * scale
    for x in range(experts):
        out_ref[x, 0] = rows[x * PART : (x + 1) * PART].astype(BF)


def slot_buffer(cotangent, expert_ids, route_weights, experts):
    tokens, width = cotangent.shape
    return pl.pallas_call(
        slots_body,
        grid=(2,),
        in_specs=[
            pl.BlockSpec((1, tokens), lambda k: (0, 0)),
            pl.BlockSpec((1, tokens), lambda k: (0, 0)),
            pl.BlockSpec((tokens, width // 2), lambda k: (0, k)),
        ],
        out_specs=pl.BlockSpec((experts, 1, PART, width // 4), lambda k: (0, k, 0, 0)),
        out_shape=jax.ShapeDtypeStruct((experts, 2, PART, width // 4), BF),
        compiler_params=PARAMS,
        cost_estimate=cost(4 * tokens * experts * PART * width, 4 * tokens * width),
        name="slots",
    )(
        *(
            pltpu.with_memory_space_constraint(value, pltpu.HBM)
            for value in (
                expert_ids.reshape(1, tokens),
                route_weights.reshape(1, tokens),
                cotangent,
            )
        )
    )


def product_body(s_ref, gate_ref, up_ref, mine_ref, theirs_ref):
    outer = s_ref[3] == 0
    for t, other in ((0, 1), (3, 2)):
        values = []
        for at in (t, other):
            gate = gate_ref[:, at].astype(F32)
            values.append(gate * jax.nn.sigmoid(gate) * up_ref[:, at].astype(F32))
        mine_ref[:, t >> 1] = jnp.where(outer, *values).astype(BF)
        theirs_ref[:, t >> 1] = jnp.where(outer, *values[::-1]).astype(BF)


def products(scalars, gate, up):
    ys, _, part, columns = gate.shape
    return pl.pallas_call(
        product_body,
        in_specs=[SCALARS, WHOLE, WHOLE],
        out_specs=[WHOLE] * 2,
        out_shape=[jax.ShapeDtypeStruct((ys, 2, part, columns), BF)] * 2,
        compiler_params=PARAMS,
        cost_estimate=cost(gate.size * 200, gate.size * 8),
        name="products",
    )(scalars, gate, up)


def picked(near, far, r1, r0):
    return jnp.where(r1 == 0, jnp.where(r0 == 0, *near), jnp.where(r0 == 0, *far))


def slot_of(e, r1, r0):
    return picked(*(((4, 0), (1, 5)) if e == 0 else ((6, 7), (3, 2))), r1, r0)


def gathered_slot(e, r1, r0):
    return picked(*(((0, 2), (5, 4)) if e == 0 else ((1, 6), (7, 3))), r1, r0)


def weight_body(s_ref, recv_ref, p0, p1, p2, p3, rows_ref, keep_ref, send_ref):
    core, a1, a0 = s_ref[0], s_ref[1], s_ref[2]
    sources = recv_ref.shape[0]
    block = keep_ref.shape[1]
    for b in range(2):
        for s in range(sources):
            rows_ref[b, s * CAP : (s + 1) * CAP, :] = recv_ref[s, b * CAP : (b + 1) * CAP, :]
    for b in range(2):
        for q, piece in enumerate((p0, p1, p2, p3)):
            grad = lax.dot_general(
                rows_ref[b], piece[...], (((0,), (0,)), ((), ())), preferred_element_type=F32
            ).astype(BF)
            low, high = grad[:block], grad[block:]
            kept = slot_of(q >> 1, (q & 1) ^ core ^ a1, b ^ a0)
            sent = slot_of(q >> 1, (q & 1) ^ core ^ a1 ^ 1, b ^ a0)
            keep_ref[kept] = jnp.where(core == 0, low, high)
            send_ref[sent] = jnp.where(core == 0, high, low)


def weight_partial(scalars, recv, pieces, block):
    sources, _, half = recv.shape
    count = sources * CAP
    columns = pieces[0].shape[1]
    grad = jax.ShapeDtypeStruct((8, block, columns), BF)
    return pl.pallas_call(
        weight_body,
        in_specs=[SCALARS] + [WHOLE] * 5,
        out_specs=[WHOLE] * 3,
        out_shape=[jax.ShapeDtypeStruct((2, count, half), BF), grad, grad],
        compiler_params=PARAMS,
        cost_estimate=cost(16 * count * half * columns, 8 * count * half),
        name="weight_partial",
    )(scalars, recv, *pieces)


def upstream_body(s_ref, rows_ref, near_ref, far_ref, *out_refs):
    core, a1, a0 = s_ref[0], s_ref[1], s_ref[2]
    for q in range(4):
        total = None
        for b in range(2):
            near = near_ref[gathered_slot(q >> 1, (q & 1) ^ core ^ a1, b ^ a0)]
            far = far_ref[gathered_slot(q >> 1, (q & 1) ^ core ^ a1 ^ 1, b ^ a0)]
            low = jnp.where(core == 0, near, far)
            high = jnp.where(core == 0, far, near)
            part = jnp.dot(
                rows_ref[b], jnp.concatenate([low, high], axis=0), preferred_element_type=F32
            )
            total = part if total is None else total + part
        out_refs[q][...] = total.astype(BF)


def upstream_partial(scalars, rows, near, far):
    _, count, half = rows.shape
    columns = near.shape[-1]
    return pl.pallas_call(
        upstream_body,
        in_specs=[SCALARS, WHOLE, WHOLE, WHOLE],
        out_specs=[WHOLE] * 4,
        out_shape=[jax.ShapeDtypeStruct((count, columns), BF)] * 4,
        compiler_params=PARAMS,
        cost_estimate=cost(16 * count * half * columns, 8 * count * half),
        name="upstream_partial",
    )(scalars, rows, near, far)


def finish_body(s_ref, gate_ref, up_ref, c0, c1, c2, c3, gate_out, up_out):
    group = s_ref[3]
    for side in range(2):
        for t in range(2):
            left, right = ((c0, c1), (c2, c3))[side]
            part = left[:, t].astype(F32) + right[:, t].astype(F32)
            index = jnp.where((group ^ side) == 0, 3 * t, 1 + t)
            gate = gate_ref[:, index].astype(F32)
            up = up_ref[:, index].astype(F32)
            sigmoid = jax.nn.sigmoid(gate)
            gate_out[:, index] = (part * up * sigmoid * (1.0 + gate * (1.0 - sigmoid))).astype(BF)
            up_out[:, index] = (part * (gate * sigmoid)).astype(BF)


def finish(scalars, gate, up, parts):
    return pl.pallas_call(
        finish_body,
        in_specs=[SCALARS] + [WHOLE] * 6,
        out_specs=[WHOLE] * 2,
        out_shape=[jax.ShapeDtypeStruct(gate.shape, BF)] * 2,
        compiler_params=PARAMS,
        cost_estimate=cost(gate.size * 200, gate.size * 12),
        name="finish",
    )(scalars, gate, up, *parts)


def added(left, right):
    return (left.astype(F32) + right.astype(F32)).astype(BF)


def dispatched(slots):
    ys = lax.axis_size("expert") // 8
    lists = [[y * 8 + z for y in range(ys) for z in zs] for zs in ((0, 1, 6, 7), (2, 3, 4, 5))]
    return lax.all_to_all(
        slots, "expert", split_axis=0, concat_axis=0, tiled=True, axis_index_groups=lists
    )


def per_device(cotangent, expert_ids, route_weights, gate_pre, up_pre, down_weight):
    devices = lax.axis_size("expert")
    experts = devices // 4
    ys = devices // 8
    columns = gate_pre.shape[1]
    block = down_weight.shape[0]
    dp = lax.axis_index("dp")
    place = lax.axis_index("expert")
    group = ((place >> 2) ^ (place >> 1)) & 1
    scalars = jnp.stack([dp & 1, dp >> 2, (dp >> 1) & 1, group]).astype(jnp.int32)
    gate4 = gate_pre.reshape(ys, 4, PART, columns)
    up4 = up_pre.reshape(ys, 4, PART, columns)

    own = [swapped(down_weight, flip, False) for flip in range(2)]
    sent = [rows.reshape(-1, columns) for rows in products(scalars, gate4, up4)]
    pieces = [sent[0]] + [expert_xor(sent[q >> 1], q) for q in (1, 2, 3)]
    slots = slot_buffer(cotangent, expert_ids, route_weights, experts)
    recv = dispatched(slots.reshape(devices // 2, PART, slots.shape[3]))
    own = [value[None] for value in own]
    ahead, behind = dp_xor(own[0], 2), dp_xor(own[1], 6)
    low = dp_xor(jnp.concatenate([own[0], ahead]), 6)
    high = dp_xor(jnp.concatenate([own[1], behind]), 2)
    near = jnp.concatenate(own + [ahead, behind, low, high])
    far = dp_xor(near, 1)

    recv, near = lax.optimization_barrier((recv, near))
    rows, keep, send = weight_partial(scalars, recv, pieces, block)
    crossed = dp_xor(send, 1)
    parts = upstream_partial(scalars, rows, near, far)
    summed = added(keep, crossed)
    first = [dp_xor(summed[0:2], 2), dp_xor(summed[2:4], 6)]
    parts = [parts[0]] + [expert_xor(parts[q], q) for q in (1, 2, 3)]
    parts = [part.reshape(ys, 2, PART, columns) for part in parts]
    first = [added(summed[4:6], first[0]), added(summed[6:8], first[1])]
    second = [dp_xor(first[0][1], 6), dp_xor(first[1][1], 2)]
    kept = [added(first[e][0], second[e]) for e in range(2)]
    weight_grad = added(swapped(kept[0], 0, True), swapped(kept[1], 1, True))
    gate_grad, up_grad = finish(scalars, gate4, up4, parts)
    return (
        weight_grad,
        gate_grad.reshape(gate_pre.shape),
        up_grad.reshape(up_pre.shape),
    )


def solution(mesh):
    placed = (
        P(("dp", "expert"), None),
        P(("dp", "expert"), None),
        P(("dp", "expert"), None),
        P("dp", "expert"),
        P("dp", "expert"),
        P("dp", "expert"),
    )
    return jax.shard_map(
        per_device,
        mesh=mesh,
        in_specs=placed,
        out_specs=(P("dp", "expert"), P("dp", "expert"), P("dp", "expert")),
        check_vma=False,
    )
```

```python
import jax
import jax.numpy as jnp
from jax import lax
from jax.experimental import pallas as pl
from jax.experimental.pallas import tpu as pltpu
from jax.sharding import PartitionSpec as P


CAP = 12
PART = 24
BF = jnp.bfloat16
F32 = jnp.float32
VMEM_LIMIT = 16 * 1024 * 1024


def expert_xor(value, mask):
    return lax.ppermute(value, "expert", [(i, i ^ mask) for i in range(lax.axis_size("expert"))])


def dp_xor(value, mask):
    return lax.ppermute(value, "dp", [(i, i ^ mask) for i in range(lax.axis_size("dp"))])


def swapped(value, flip, back):
    experts = lax.axis_size("expert")
    pairs = []
    for d in range(lax.axis_size("dp")):
        for s in range(experts):
            high = d >> 2
            to_dp = ((s & 1) ^ high ^ (d & 1)) * 4 + (d & 3)
            to_expert = (s & ~3) + (((s >> 1) & 1) ^ flip) * 2 + high
            pairs.append((d * experts + s, to_dp * experts + to_expert))
    if back:
        pairs = [(target, source) for source, target in pairs]
    return lax.ppermute(value, ("dp", "expert"), pairs)


SCALARS = pl.BlockSpec(memory_space=pltpu.SMEM)
WHOLE = pl.BlockSpec(memory_space=pltpu.VMEM)
PARAMS = pltpu.CompilerParams(vmem_limit_bytes=VMEM_LIMIT)


def cost(flops, size):
    return pl.CostEstimate(flops=flops, transcendentals=0, bytes_accessed=size)


def slots_body(ids_ref, weights_ref, cot_ref, out_ref):
    tokens = ids_ref.shape[1]
    experts = out_ref.shape[0]
    half = out_ref.shape[3]
    ids = jnp.broadcast_to(ids_ref[...].astype(F32), (tokens, tokens))
    row = lax.broadcasted_iota(jnp.int32, (tokens, tokens), 0)
    col = lax.broadcasted_iota(jnp.int32, (tokens, tokens), 1)
    ids_down = jnp.sum(jnp.where(row == col, ids, 0.0), axis=1, keepdims=True)
    earlier = jnp.where((ids_down == ids) & (row < col), 1.0, 0.0)
    position = jnp.sum(earlier, axis=0, keepdims=True)
    target = (ids_ref[...].astype(F32) * PART + position).astype(jnp.int32)
    place = lax.broadcasted_iota(jnp.int32, (experts * PART, tokens), 0)
    first = place == target
    second = place == target + CAP
    scale = jnp.sum(jnp.where(first | second, weights_ref[...], 0.0), axis=1, keepdims=True)
    picked = jnp.dot(
        first.astype(F32).astype(BF), cot_ref[:, :half], preferred_element_type=F32
    ) + jnp.dot(second.astype(F32).astype(BF), cot_ref[:, half:], preferred_element_type=F32)
    rows = picked * scale
    for x in range(experts):
        out_ref[x, 0] = rows[x * PART : (x + 1) * PART].astype(BF)


def slot_buffer(cotangent, expert_ids, route_weights, experts):
    tokens, width = cotangent.shape
    return pl.pallas_call(
        slots_body,
        grid=(2,),
        in_specs=[
            pl.BlockSpec((1, tokens), lambda k: (0, 0)),
            pl.BlockSpec((1, tokens), lambda k: (0, 0)),
            pl.BlockSpec((tokens, width // 2), lambda k: (0, k)),
        ],
        out_specs=pl.BlockSpec((experts, 1, PART, width // 4), lambda k: (0, k, 0, 0)),
        out_shape=jax.ShapeDtypeStruct((experts, 2, PART, width // 4), BF),
        compiler_params=PARAMS,
        cost_estimate=cost(4 * tokens * experts * PART * width, 4 * tokens * width),
        name="slots",
    )(
        *(
            pltpu.with_memory_space_constraint(value, pltpu.HBM)
            for value in (
                expert_ids.reshape(1, tokens),
                route_weights.reshape(1, tokens),
                cotangent,
            )
        )
    )


def product_body(s_ref, gate_ref, up_ref, mine_ref, theirs_ref):
    outer = s_ref[3] == 0
    for t, other in ((0, 1), (3, 2)):
        values = []
        for at in (t, other):
            gate = gate_ref[:, at].astype(F32)
            values.append(gate * jax.nn.sigmoid(gate) * up_ref[:, at].astype(F32))
        mine_ref[:, t >> 1] = jnp.where(outer, *values).astype(BF)
        theirs_ref[:, t >> 1] = jnp.where(outer, *values[::-1]).astype(BF)


def products(scalars, gate, up):
    ys, _, part, columns = gate.shape
    return pl.pallas_call(
        product_body,
        in_specs=[SCALARS, WHOLE, WHOLE],
        out_specs=[WHOLE] * 2,
        out_shape=[jax.ShapeDtypeStruct((ys, 2, part, columns), BF)] * 2,
        compiler_params=PARAMS,
        cost_estimate=cost(gate.size * 200, gate.size * 8),
        name="products",
    )(scalars, gate, up)


def picked(near, far, r1, r0):
    return jnp.where(r1 == 0, jnp.where(r0 == 0, *near), jnp.where(r0 == 0, *far))


def slot_of(e, r1, r0):
    return picked(*(((4, 0), (1, 5)) if e == 0 else ((6, 7), (3, 2))), r1, r0)


def gathered_slot(e, r1, r0):
    return picked(*(((0, 2), (5, 4)) if e == 0 else ((1, 6), (7, 3))), r1, r0)


def weight_body(s_ref, recv_ref, p0, p1, p2, p3, rows_ref, keep_ref, send_ref):
    core, a1, a0 = s_ref[0], s_ref[1], s_ref[2]
    sources = recv_ref.shape[0]
    block = keep_ref.shape[1]
    for b in range(2):
        for s in range(sources):
            rows_ref[b, s * CAP : (s + 1) * CAP, :] = recv_ref[s, b * CAP : (b + 1) * CAP, :]
    for b in range(2):
        for q, piece in enumerate((p0, p1, p2, p3)):
            grad = lax.dot_general(
                rows_ref[b], piece[...], (((0,), (0,)), ((), ())), preferred_element_type=F32
            ).astype(BF)
            low, high = grad[:block], grad[block:]
            kept = slot_of(q >> 1, (q & 1) ^ core ^ a1, b ^ a0)
            sent = slot_of(q >> 1, (q & 1) ^ core ^ a1 ^ 1, b ^ a0)
            keep_ref[kept] = jnp.where(core == 0, low, high)
            send_ref[sent] = jnp.where(core == 0, high, low)


def weight_partial(scalars, recv, pieces, block):
    sources, _, half = recv.shape
    count = sources * CAP
    columns = pieces[0].shape[1]
    grad = jax.ShapeDtypeStruct((8, block, columns), BF)
    return pl.pallas_call(
        weight_body,
        in_specs=[SCALARS] + [WHOLE] * 5,
        out_specs=[WHOLE] * 3,
        out_shape=[jax.ShapeDtypeStruct((2, count, half), BF), grad, grad],
        compiler_params=PARAMS,
        cost_estimate=cost(16 * count * half * columns, 8 * count * half),
        name="weight_partial",
    )(scalars, recv, *pieces)


def upstream_body(s_ref, rows_ref, near_ref, far_ref, *out_refs):
    core, a1, a0 = s_ref[0], s_ref[1], s_ref[2]
    for q in range(4):
        total = None
        for b in range(2):
            near = near_ref[gathered_slot(q >> 1, (q & 1) ^ core ^ a1, b ^ a0)]
            far = far_ref[gathered_slot(q >> 1, (q & 1) ^ core ^ a1 ^ 1, b ^ a0)]
            low = jnp.where(core == 0, near, far)
            high = jnp.where(core == 0, far, near)
            part = jnp.dot(
                rows_ref[b], jnp.concatenate([low, high], axis=0), preferred_element_type=F32
            )
            total = part if total is None else total + part
        out_refs[q][...] = total.astype(BF)


def upstream_partial(scalars, rows, near, far):
    _, count, half = rows.shape
    columns = near.shape[-1]
    return pl.pallas_call(
        upstream_body,
        in_specs=[SCALARS, WHOLE, WHOLE, WHOLE],
        out_specs=[WHOLE] * 4,
        out_shape=[jax.ShapeDtypeStruct((count, columns), BF)] * 4,
        compiler_params=PARAMS,
        cost_estimate=cost(16 * count * half * columns, 8 * count * half),
        name="upstream_partial",
    )(scalars, rows, near, far)


def finish_body(s_ref, gate_ref, up_ref, c0, c1, c2, c3, gate_out, up_out):
    group = s_ref[3]
    for side in range(2):
        for t in range(2):
            left, right = ((c0, c1), (c2, c3))[side]
            part = left[:, t].astype(F32) + right[:, t].astype(F32)
            index = jnp.where((group ^ side) == 0, 3 * t, 1 + t)
            gate = gate_ref[:, index].astype(F32)
            up = up_ref[:, index].astype(F32)
            sigmoid = jax.nn.sigmoid(gate)
            gate_out[:, index] = (part * up * sigmoid * (1.0 + gate * (1.0 - sigmoid))).astype(BF)
            up_out[:, index] = (part * (gate * sigmoid)).astype(BF)


def finish(scalars, gate, up, parts):
    return pl.pallas_call(
        finish_body,
        in_specs=[SCALARS] + [WHOLE] * 6,
        out_specs=[WHOLE] * 2,
        out_shape=[jax.ShapeDtypeStruct(gate.shape, BF)] * 2,
        compiler_params=PARAMS,
        cost_estimate=cost(gate.size * 200, gate.size * 12),
        name="finish",
    )(scalars, gate, up, *parts)


def added(left, right):
    return (left.astype(F32) + right.astype(F32)).astype(BF)


def dispatched(slots):
    ys = lax.axis_size("expert") // 8
    lists = [[y * 8 + z for y in range(ys) for z in zs] for zs in ((0, 1, 6, 7), (2, 3, 4, 5))]
    return lax.all_to_all(
        slots, "expert", split_axis=0, concat_axis=0, tiled=True, axis_index_groups=lists
    )


def per_device(cotangent, expert_ids, route_weights, gate_pre, up_pre, down_weight):
    devices = lax.axis_size("expert")
    experts = devices // 4
    ys = devices // 8
    columns = gate_pre.shape[1]
    block = down_weight.shape[0]
    dp = lax.axis_index("dp")
    place = lax.axis_index("expert")
    group = ((place >> 2) ^ (place >> 1)) & 1
    scalars = jnp.stack([dp & 1, dp >> 2, (dp >> 1) & 1, group]).astype(jnp.int32)
    gate4 = gate_pre.reshape(ys, 4, PART, columns)
    up4 = up_pre.reshape(ys, 4, PART, columns)

    own = [swapped(down_weight, flip, False) for flip in range(2)]
    sent = [rows.reshape(-1, columns) for rows in products(scalars, gate4, up4)]
    pieces = [sent[0]] + [expert_xor(sent[q >> 1], q) for q in (1, 2, 3)]
    slots = slot_buffer(cotangent, expert_ids, route_weights, experts)
    recv = dispatched(slots.reshape(devices // 2, PART, slots.shape[3]))
    own = [value[None] for value in own]
    ahead, behind = dp_xor(own[0], 2), dp_xor(own[1], 6)
    low = dp_xor(jnp.concatenate([own[0], ahead]), 6)
    high = dp_xor(jnp.concatenate([own[1], behind]), 2)
    near = jnp.concatenate(own + [ahead, behind, low, high])
    far = dp_xor(near, 1)

    recv, near = lax.optimization_barrier((recv, near))
    rows, keep, send = weight_partial(scalars, recv, pieces, block)
    crossed = dp_xor(send, 1)
    parts = upstream_partial(scalars, rows, near, far)
    summed = added(keep, crossed)
    far_sum = dp_xor(summed[2:4], 6)
    near_sum = dp_xor(summed[0:2], 2)
    parts = [parts[0]] + [expert_xor(parts[q], q) for q in (1, 2, 3)]
    parts = [part.reshape(ys, 2, PART, columns) for part in parts]
    far_first = added(summed[6:8], far_sum)
    near_sum, far_first = lax.optimization_barrier((near_sum, far_first))
    near_first = added(summed[4:6], near_sum)
    far_second = dp_xor(far_first[1], 2)
    near_second = dp_xor(near_first[1], 6)
    crossed = swapped(added(far_first[0], far_second), 1, True)
    stayed = swapped(added(near_first[0], near_second), 0, True)
    weight_grad = added(stayed, crossed)
    gate_grad, up_grad = finish(scalars, gate4, up4, parts)
    return (
        weight_grad,
        gate_grad.reshape(gate_pre.shape),
        up_grad.reshape(up_pre.shape),
    )


def solution(mesh):
    placed = (
        P(("dp", "expert"), None),
        P(("dp", "expert"), None),
        P(("dp", "expert"), None),
        P("dp", "expert"),
        P("dp", "expert"),
        P("dp", "expert"),
    )
    return jax.shard_map(
        per_device,
        mesh=mesh,
        in_specs=placed,
        out_specs=(P("dp", "expert"), P("dp", "expert"), P("dp", "expert")),
        check_vma=False,
    )
```

```python
import jax
import jax.numpy as jnp
from jax import lax
from jax.experimental import pallas as pl
from jax.experimental.pallas import tpu as pltpu
from jax.sharding import PartitionSpec as P


CAP = 12
PART = 24
BF = jnp.bfloat16
F32 = jnp.float32
VMEM_LIMIT = 16 * 1024 * 1024


def expert_xor(value, mask):
    return lax.ppermute(value, "expert", [(i, i ^ mask) for i in range(lax.axis_size("expert"))])


def dp_xor(value, mask):
    return lax.ppermute(value, "dp", [(i, i ^ mask) for i in range(lax.axis_size("dp"))])


def swapped(value, flip, back):
    experts = lax.axis_size("expert")
    pairs = []
    for d in range(lax.axis_size("dp")):
        for s in range(experts):
            high = d >> 2
            to_dp = ((s & 1) ^ high ^ (d & 1)) * 4 + (d & 3)
            to_expert = (s & ~3) + (((s >> 1) & 1) ^ flip) * 2 + high
            pairs.append((d * experts + s, to_dp * experts + to_expert))
    if back:
        pairs = [(target, source) for source, target in pairs]
    return lax.ppermute(value, ("dp", "expert"), pairs)


SCALARS = pl.BlockSpec(memory_space=pltpu.SMEM)
WHOLE = pl.BlockSpec(memory_space=pltpu.VMEM)
PARAMS = pltpu.CompilerParams(vmem_limit_bytes=VMEM_LIMIT)


def cost(flops, size):
    return pl.CostEstimate(flops=flops, transcendentals=0, bytes_accessed=size)


def slots_body(ids_ref, weights_ref, cot_ref, out_ref):
    tokens = ids_ref.shape[1]
    experts = out_ref.shape[0]
    half = out_ref.shape[3]
    ids = jnp.broadcast_to(ids_ref[...].astype(F32), (tokens, tokens))
    row = lax.broadcasted_iota(jnp.int32, (tokens, tokens), 0)
    col = lax.broadcasted_iota(jnp.int32, (tokens, tokens), 1)
    ids_down = jnp.sum(jnp.where(row == col, ids, 0.0), axis=1, keepdims=True)
    earlier = jnp.where((ids_down == ids) & (row < col), 1.0, 0.0)
    position = jnp.sum(earlier, axis=0, keepdims=True)
    target = (ids_ref[...].astype(F32) * PART + position).astype(jnp.int32)
    place = lax.broadcasted_iota(jnp.int32, (experts * PART, tokens), 0)
    first = place == target
    second = place == target + CAP
    scale = jnp.sum(jnp.where(first | second, weights_ref[...], 0.0), axis=1, keepdims=True)
    picked = jnp.dot(
        first.astype(F32).astype(BF), cot_ref[:, :half], preferred_element_type=F32
    ) + jnp.dot(second.astype(F32).astype(BF), cot_ref[:, half:], preferred_element_type=F32)
    rows = picked * scale
    for x in range(experts):
        out_ref[x, 0] = rows[x * PART : (x + 1) * PART].astype(BF)


def slot_buffer(cotangent, expert_ids, route_weights, experts):
    tokens, width = cotangent.shape
    return pl.pallas_call(
        slots_body,
        grid=(2,),
        in_specs=[
            pl.BlockSpec((1, tokens), lambda k: (0, 0)),
            pl.BlockSpec((1, tokens), lambda k: (0, 0)),
            pl.BlockSpec((tokens, width // 2), lambda k: (0, k)),
        ],
        out_specs=pl.BlockSpec((experts, 1, PART, width // 4), lambda k: (0, k, 0, 0)),
        out_shape=jax.ShapeDtypeStruct((experts, 2, PART, width // 4), BF),
        compiler_params=PARAMS,
        cost_estimate=cost(4 * tokens * experts * PART * width, 4 * tokens * width),
        name="slots",
    )(
        *(
            pltpu.with_memory_space_constraint(value, pltpu.HBM)
            for value in (
                expert_ids.reshape(1, tokens),
                route_weights.reshape(1, tokens),
                cotangent,
            )
        )
    )


def product_body(s_ref, gate_ref, up_ref, mine_ref, theirs_ref):
    outer = s_ref[3] == 0
    for t, other in ((0, 1), (3, 2)):
        values = []
        for at in (t, other):
            gate = gate_ref[:, at].astype(F32)
            values.append(gate * jax.nn.sigmoid(gate) * up_ref[:, at].astype(F32))
        mine_ref[:, t >> 1] = jnp.where(outer, *values).astype(BF)
        theirs_ref[:, t >> 1] = jnp.where(outer, *values[::-1]).astype(BF)


def products(scalars, gate, up):
    ys, _, part, columns = gate.shape
    return pl.pallas_call(
        product_body,
        in_specs=[SCALARS, WHOLE, WHOLE],
        out_specs=[WHOLE] * 2,
        out_shape=[jax.ShapeDtypeStruct((ys, 2, part, columns), BF)] * 2,
        compiler_params=PARAMS,
        cost_estimate=cost(gate.size * 200, gate.size * 8),
        name="products",
    )(scalars, gate, up)


def picked(near, far, r1, r0):
    return jnp.where(r1 == 0, jnp.where(r0 == 0, *near), jnp.where(r0 == 0, *far))


def slot_of(e, r1, r0):
    return picked(*(((4, 0), (1, 5)) if e == 0 else ((6, 7), (3, 2))), r1, r0)


def gathered_slot(e, r1, r0):
    return picked(*(((0, 2), (5, 4)) if e == 0 else ((1, 6), (7, 3))), r1, r0)


def weight_body(s_ref, recv_ref, p0, p1, p2, p3, rows_ref, keep_ref, send_ref):
    core, a1, a0 = s_ref[0], s_ref[1], s_ref[2]
    sources = recv_ref.shape[0]
    block = keep_ref.shape[1]
    for b in range(2):
        for s in range(sources):
            rows_ref[b, s * CAP : (s + 1) * CAP, :] = recv_ref[s, b * CAP : (b + 1) * CAP, :]
    for b in range(2):
        for q, piece in enumerate((p0, p1, p2, p3)):
            grad = lax.dot_general(
                rows_ref[b], piece[...], (((0,), (0,)), ((), ())), preferred_element_type=F32
            ).astype(BF)
            low, high = grad[:block], grad[block:]
            kept = slot_of(q >> 1, (q & 1) ^ core ^ a1, b ^ a0)
            sent = slot_of(q >> 1, (q & 1) ^ core ^ a1 ^ 1, b ^ a0)
            keep_ref[kept] = jnp.where(core == 0, low, high)
            send_ref[sent] = jnp.where(core == 0, high, low)


def weight_partial(scalars, recv, pieces, block):
    sources, _, half = recv.shape
    count = sources * CAP
    columns = pieces[0].shape[1]
    grad = jax.ShapeDtypeStruct((8, block, columns), BF)
    return pl.pallas_call(
        weight_body,
        in_specs=[SCALARS] + [WHOLE] * 5,
        out_specs=[WHOLE] * 3,
        out_shape=[jax.ShapeDtypeStruct((2, count, half), BF), grad, grad],
        compiler_params=PARAMS,
        cost_estimate=cost(16 * count * half * columns, 8 * count * half),
        name="weight_partial",
    )(scalars, recv, *pieces)


def stacked_body(*refs):
    at = 0
    for ref in refs[:-1]:
        refs[-1][at : at + ref.shape[0]] = ref[...]
        at += ref.shape[0]


def stacked(values):
    total = sum(value.shape[0] for value in values)
    return pl.pallas_call(
        stacked_body,
        in_specs=[WHOLE] * len(values),
        out_specs=WHOLE,
        out_shape=jax.ShapeDtypeStruct((total, *values[0].shape[1:]), BF),
        compiler_params=pltpu.CompilerParams(vmem_limit_bytes=VMEM_LIMIT // 4),
        cost_estimate=cost(values[0].size * 8, values[0].size * 32),
        name="stacked",
    )(*values)


def upstream_body(s_ref, rows_ref, near_ref, far_ref, *out_refs):
    core, a1, a0 = s_ref[0], s_ref[1], s_ref[2]
    for q in range(4):
        total = None
        for b in range(2):
            near = near_ref[gathered_slot(q >> 1, (q & 1) ^ core ^ a1, b ^ a0)]
            far = far_ref[gathered_slot(q >> 1, (q & 1) ^ core ^ a1 ^ 1, b ^ a0)]
            low = jnp.where(core == 0, near, far)
            high = jnp.where(core == 0, far, near)
            part = jnp.dot(
                rows_ref[b], jnp.concatenate([low, high], axis=0), preferred_element_type=F32
            )
            total = part if total is None else total + part
        out_refs[q][...] = total.astype(BF)


def upstream_partial(scalars, rows, near, far):
    _, count, half = rows.shape
    columns = near.shape[-1]
    return pl.pallas_call(
        upstream_body,
        in_specs=[SCALARS, WHOLE, WHOLE, WHOLE],
        out_specs=[WHOLE] * 4,
        out_shape=[jax.ShapeDtypeStruct((count, columns), BF)] * 4,
        compiler_params=PARAMS,
        cost_estimate=cost(16 * count * half * columns, 8 * count * half),
        name="upstream_partial",
    )(scalars, rows, near, far)


def finish_body(s_ref, gate_ref, up_ref, c0, c1, c2, c3, gate_out, up_out):
    group = s_ref[3]
    for side in range(2):
        for t in range(2):
            left, right = ((c0, c1), (c2, c3))[side]
            part = left[:, t].astype(F32) + right[:, t].astype(F32)
            index = jnp.where((group ^ side) == 0, 3 * t, 1 + t)
            gate = gate_ref[:, index].astype(F32)
            up = up_ref[:, index].astype(F32)
            sigmoid = jax.nn.sigmoid(gate)
            gate_out[:, index] = (part * up * sigmoid * (1.0 + gate * (1.0 - sigmoid))).astype(BF)
            up_out[:, index] = (part * (gate * sigmoid)).astype(BF)


def finish(scalars, gate, up, parts):
    return pl.pallas_call(
        finish_body,
        in_specs=[SCALARS] + [WHOLE] * 6,
        out_specs=[WHOLE] * 2,
        out_shape=[jax.ShapeDtypeStruct(gate.shape, BF)] * 2,
        compiler_params=PARAMS,
        cost_estimate=cost(gate.size * 200, gate.size * 12),
        name="finish",
    )(scalars, gate, up, *parts)


def added(left, right):
    return (left.astype(F32) + right.astype(F32)).astype(BF)


def dispatched(slots):
    ys = lax.axis_size("expert") // 8
    lists = [[y * 8 + z for y in range(ys) for z in zs] for zs in ((0, 1, 6, 7), (2, 3, 4, 5))]
    return lax.all_to_all(
        slots, "expert", split_axis=0, concat_axis=0, tiled=True, axis_index_groups=lists
    )


def per_device(cotangent, expert_ids, route_weights, gate_pre, up_pre, down_weight):
    devices = lax.axis_size("expert")
    experts = devices // 4
    ys = devices // 8
    columns = gate_pre.shape[1]
    block = down_weight.shape[0]
    dp = lax.axis_index("dp")
    place = lax.axis_index("expert")
    group = ((place >> 2) ^ (place >> 1)) & 1
    scalars = jnp.stack([dp & 1, dp >> 2, (dp >> 1) & 1, group]).astype(jnp.int32)
    gate4 = gate_pre.reshape(ys, 4, PART, columns)
    up4 = up_pre.reshape(ys, 4, PART, columns)

    own = [swapped(down_weight, flip, False) for flip in range(2)]
    sent = [rows.reshape(-1, columns) for rows in products(scalars, gate4, up4)]
    pieces = [sent[0]] + [expert_xor(sent[q >> 1], q) for q in (1, 2, 3)]
    slots = slot_buffer(cotangent, expert_ids, route_weights, experts)
    recv = dispatched(slots.reshape(devices // 2, PART, slots.shape[3]))
    own = [value[None] for value in own]
    ahead, behind = dp_xor(own[0], 2), dp_xor(own[1], 6)
    low = dp_xor(stacked([own[0], ahead]), 6)
    high = dp_xor(stacked([own[1], behind]), 2)
    near = jnp.concatenate(own + [ahead, behind, low, high])
    far = dp_xor(near, 1)

    recv, near = lax.optimization_barrier((recv, near))
    rows, keep, send = weight_partial(scalars, recv, pieces, block)
    crossed = dp_xor(send, 1)
    parts = upstream_partial(scalars, rows, near, far)
    summed = added(keep, crossed)
    first = [dp_xor(summed[0:2], 2), dp_xor(summed[2:4], 6)]
    parts = [parts[0]] + [expert_xor(parts[q], q) for q in (1, 2, 3)]
    parts = [part.reshape(ys, 2, PART, columns) for part in parts]
    first = [added(summed[4:6], first[0]), added(summed[6:8], first[1])]
    second = [dp_xor(first[0][1], 6), dp_xor(first[1][1], 2)]
    kept = [added(first[e][0], second[e]) for e in range(2)]
    weight_grad = added(swapped(kept[0], 0, True), swapped(kept[1], 1, True))
    gate_grad, up_grad = finish(scalars, gate4, up4, parts)
    return (
        weight_grad,
        gate_grad.reshape(gate_pre.shape),
        up_grad.reshape(up_pre.shape),
    )


def solution(mesh):
    placed = (
        P(("dp", "expert"), None),
        P(("dp", "expert"), None),
        P(("dp", "expert"), None),
        P("dp", "expert"),
        P("dp", "expert"),
        P("dp", "expert"),
    )
    return jax.shard_map(
        per_device,
        mesh=mesh,
        in_specs=placed,
        out_specs=(P("dp", "expert"), P("dp", "expert"), P("dp", "expert")),
        check_vma=False,
    )
```
